256 devices in a mesh: bank: 8 (over y, x_lo), zero: 32 (over z, x_hi, core).
Axes of the slice: x: 4 (x_hi: 2, x_lo: 2; x = x_hi * 2 + x_lo), y: 4, z: 8, core: 2. Of those that a mesh axis runs over, the one named last changes fastest.
Arguments:
- master_gate: float32 [64, 2048, 1024], P('bank', 'zero'), may hold values from -0.25 to 0.25
- master_up: float32 [64, 2048, 1024], P('bank', 'zero'), may hold values from -0.25 to 0.25
- master_down: float32 [64, 1024, 2048], P('bank', None, 'zero'), may hold values from -0.375 to 0.375
- router_weight: float32 [2048, 64], P('zero', 'bank'), may hold values from -0.125 to 0.125
- router_gain: float32 [2048], P('zero'), may hold values from 0.25 to 1.75
Outputs:
- final_gate: bfloat16 [64, 2048, 1024], P('bank', None, 'zero')
- final_up: bfloat16 [64, 2048, 1024], P('bank', None, 'zero')
- final_down: bfloat16 [64, 1024, 2048], P('bank', 'zero')
- scale_gate: float32 [64, 1024], P('bank', 'zero')
- scale_up: float32 [64, 1024], P('bank', 'zero')
- scale_down: float32 [64, 1024], P('bank', 'zero')
- serve_router: bfloat16 [2048, 64], replicated
The draws below stay inside these ranges and needn't reach their ends.
All inputs are finite; a program needn't handle non-finite values.
Results may differ from the reference program's by a relative error of at most 0.0085.
Values may be sent and summed in bfloat16 or wider, within the bound.
A program may use at most 64 MiB of HBM per device.

```python
import jax
import jax.numpy as jnp
from jax import lax

EXPERTS = 64
D_MODEL = 2048
D_EXPERT = 1024


def raised(values, own_key, source, target, shards_of, factor):
    owner, partner = [(jnp.arange(values.shape[position]) // (values.shape[position] // shards_of)).reshape([-1 if axis == position else 1 for axis in range(values.ndim)]) for position in (source, target)]
    chosen = jax.random.permutation(own_key, shards_of)[partner]
    strong = (owner == chosen) | (owner == (partner + shards_of // 2) % shards_of)
    return jnp.where(strong, factor * values, values)


def block_levels(own_key, shape, pieces, low, largest):
    gain, own = 1.0, jax.random.fold_in(own_key, 6)
    for axis_at, parts in pieces:
        draws = jnp.exp(jax.random.uniform(jax.random.fold_in(own, axis_at), (parts,), jnp.float32, low / len(pieces), largest / len(pieces)))
        gain = gain * jnp.repeat(draws, shape[axis_at] // parts).reshape([-1 if axis == axis_at else 1 for axis in range(len(shape))])
    return gain


def centred(stream_key, shape, width, limit, split=(), dtype=jnp.bfloat16):
    array = jax.random.normal(stream_key, shape, jnp.float32) * width
    if len(split) > 0:
        array = block_levels(stream_key, shape, split, -0.22, 0.18) * array
    return jnp.clip(array, min=-limit, max=limit).astype(dtype)


def gaussian_with(rng, extent, width, reach, pieces, heavy, held_as=jnp.bfloat16):
    drawn = width * jax.random.normal(rng, extent, jnp.float32)
    if pieces:
        drawn = drawn * block_levels(rng, extent, pieces, -0.22, 0.18)
    return jnp.clip(raised(drawn, jax.random.fold_in(rng, 3), *heavy), -reach, reach).astype(held_as)


def setup_inputs(seed: int = 0) -> dict:
    seeds = jax.random.split(jax.random.key(seed), 6)
    master_gate = gaussian_with(seeds[0], (EXPERTS, D_MODEL, D_EXPERT), D_MODEL ** -0.5, 0.25, ((0, 8), (1, 32)), (1, 2, 32, 2.75), jnp.float32)
    master_up = gaussian_with(seeds[1], (EXPERTS, D_MODEL, D_EXPERT), D_MODEL ** -0.5, 0.25, ((0, 8), (1, 32)), (1, 2, 32, 2.75), jnp.float32)
    master_down = gaussian_with(seeds[2], (EXPERTS, D_EXPERT, D_MODEL), D_EXPERT ** -0.5, 0.375, ((0, 8), (2, 32)), (2, 1, 32, 2.75), jnp.float32)
    router_weight = centred(seeds[3], (D_MODEL, EXPERTS), D_MODEL ** -0.5, 0.125, ((0, 32), (1, 8)), jnp.float32)
    router_gain = jnp.clip(1.0 + 0.15 * jax.random.normal(seeds[4], (D_MODEL,), jnp.float32), 0.25, 1.75)
    return dict(master_gate=master_gate, master_up=master_up, master_down=master_down, router_weight=router_weight, router_gain=router_gain)


def reference(master_gate, master_up, master_down, router_weight, router_gain):
    scale_gate = jnp.sqrt(lax.optimization_barrier(jnp.sum(master_gate * master_gate, axis=1)))
    final_gate = (master_gate / jnp.expand_dims(scale_gate, 1)).astype(jnp.bfloat16)
    scale_up = jnp.sqrt(lax.optimization_barrier(jnp.sum(master_up * master_up, axis=1)))
    final_up = (master_up / jnp.expand_dims(scale_up, 1)).astype(jnp.bfloat16)
    scale_down = jnp.sqrt(lax.optimization_barrier(jnp.sum(master_down * master_down, axis=2)))
    final_down = (master_down / jnp.expand_dims(scale_down, 2)).astype(jnp.bfloat16)
    serve_router = (router_weight * router_gain[:, None]).astype(jnp.bfloat16)
    return (final_gate, final_up, final_down, scale_gate, scale_up, scale_down, serve_router)
```

```python
import functools

import jax
import jax.numpy as jnp
from jax import lax
from jax.experimental import pallas as pl
from jax.experimental.pallas import tpu as pltpu
from jax.sharding import PartitionSpec as P

MESH = pl.DeviceIdType.MESH
ZERO, BANK = 32, 8
CHIPS = ZERO // 2
HEADS = 8
PAIRS = 12
ROWS, COLS, PIECE, LANES = 64, 1024, 32, 128


def zero_peer(me, step):
    z, x, core = me // 4, (me // 2) % 2, me % 2
    turn = step // 4
    away = (turn + 1) // 2
    dz = jnp.where(turn % 2 == 1, 4 - away, 4 + away)
    dx = 1 - (step // 2) % 2
    dc = 1 - step % 2
    return ((z + dz) % 8) * 4 + ((x + dx) % 2) * 2 + (core + dc) % 2


def exchange(
    gate, up, down, router_hbm, gain_hbm,
    final, scales, served,
    held, router, gain, send, recv, mine, other, rows,
    load_sem, send_sem, recv_sem, own_sem, pair_sem, row_sem, bank_sem, small_sem,
):
    me, bank = lax.axis_index("zero"), lax.axis_index("bank")
    core, chip = me % 2, me // 2
    sources = (gate, up, down)

    def load(p):
        source = sources[p // 4]
        return pltpu.make_async_copy(source.at[pl.ds((p % 4) * LANES, LANES)], held.at[p], load_sem.at[p])

    load(0).start()
    small = (
        pltpu.make_async_copy(router_hbm, router, small_sem.at[0]),
        pltpu.make_async_copy(gain_hbm, gain, small_sem.at[1]),
    )
    for copy in small:
        copy.start()
    for p in range(1, PAIRS):
        load(p).start()

    barrier = pltpu.get_barrier_semaphore()

    def greet(step, _):
        pl.semaphore_signal(barrier, inc=1, device_id={"zero": zero_peer(me, step)}, device_id_type=MESH)
        return 0

    lax.fori_loop(0, ZERO - 1, greet, 0)
    for step in range(1, BANK):
        pl.semaphore_signal(barrier, inc=1, device_id={"bank": (bank + step) % BANK}, device_id_type=MESH)

    half = lax.broadcasted_iota(jnp.int32, (PIECE, LANES), 1) < ROWS
    for copy in small:
        copy.wait()
    part = (router[...] * gain[...]).astype(jnp.bfloat16)
    mine[...] = jnp.concatenate([part, part], axis=1)

    def prepare(p):
        def block(q, _):
            at = pl.multiple_of(q * LANES, LANES)
            turned = held[p, :, pl.ds(at, LANES)].T.astype(jnp.bfloat16)
            send[p, pl.ds(q * 4, 4)] = turned.reshape(4, PIECE, LANES)
            return 0

        lax.fori_loop(0, COLS // LANES, block, 0)

    def start(p):
        def one(step, _):
            peer = zero_peer(me, step)
            pltpu.make_async_remote_copy(
                src_ref=send.at[p, peer], dst_ref=recv.at[p, me], send_sem=send_sem.at[p],
                recv_sem=recv_sem.at[p], device_id={"zero": peer}, device_id_type=MESH,
            ).start()
            return 0

        lax.fori_loop(0, ZERO - 1, one, 0)
        pltpu.make_async_copy(send.at[p, me], recv.at[p, me], own_sem.at[p]).start()

    load(0).wait()
    prepare(0)
    pl.semaphore_wait(barrier, ZERO - 1 + BANK - 1)

    to_pair = pltpu.make_async_remote_copy(
        src_ref=mine, dst_ref=other, send_sem=pair_sem.at[0], recv_sem=pair_sem.at[1],
        device_id={"zero": chip * 2 + 1 - core}, device_id_type=MESH,
    )
    to_pair.start()
    start(0)

    to_pair.wait()
    lower = lax.broadcasted_iota(jnp.int32, (HEADS, LANES), 1) < ROWS
    keep_mine = jnp.where(lower, 0, 1) == core
    at_chip = pl.ds(pl.multiple_of(chip * LANES, LANES), LANES)
    rows[:, at_chip] = jnp.where(
        keep_mine, mine[...].astype(jnp.float32), other[...].astype(jnp.float32)
    ).astype(jnp.bfloat16)

    def row_copy(step):
        return pltpu.make_async_remote_copy(
            src_ref=rows.at[:, at_chip], dst_ref=rows.at[:, at_chip], send_sem=row_sem.at[0],
            recv_sem=row_sem.at[1], device_id={"zero": ((chip + step) % CHIPS) * 2 + core}, device_id_type=MESH,
        )

    for step in range(1, CHIPS):
        row_copy(step).start()

    for p in range(1, PAIRS):
        load(p).wait()
        prepare(p)
        start(p)

    others = rows.at[:, pl.ds(0, (CHIPS - 1) * LANES)]
    pltpu.make_async_copy(others, others, row_sem.at[1]).wait()

    def bank_copy(step):
        return pltpu.make_async_remote_copy(
            src_ref=rows, dst_ref=served.at[bank], send_sem=bank_sem.at[0],
            recv_sem=bank_sem.at[1], device_id={"bank": (bank + step) % BANK}, device_id_type=MESH,
        )

    for step in range(1, BANK):
        bank_copy(step).start()
    served[bank] = rows[...]

    lane = lax.broadcasted_iota(jnp.int32, (PIECE, LANES), 1)

    def finish(p, kept):
        pltpu.make_async_copy(send.at[p, me], recv.at[p, me], own_sem.at[p]).wait()
        arrived = pltpu.make_async_copy(recv.at[p, pl.ds(0, ZERO - 1)], recv.at[p, pl.ds(0, ZERO - 1)], recv_sem.at[p])
        arrived.wait()

        def square(k, total):
            a = recv[p, 2 * k].astype(jnp.float32)
            b = recv[p, 2 * k + 1].astype(jnp.float32)
            return total + (a * a + b * b)

        total = lax.fori_loop(0, CHIPS, square, jnp.zeros((PIECE, LANES), jnp.float32), unroll=4)
        first = jnp.sqrt(jnp.sum(jnp.where(half, total, 0.0), axis=1, keepdims=True))
        second = jnp.sqrt(jnp.sum(jnp.where(half, 0.0, total), axis=1, keepdims=True))
        factor = 1.0 / jnp.where(half, first, second)

        def spread(k, _):
            a = recv[p, 2 * k].astype(jnp.float32) * factor
            b = recv[p, 2 * k + 1].astype(jnp.float32) * factor
            at = pl.ds(pl.multiple_of(k * LANES, LANES), LANES)
            final[2 * p, :, at] = jnp.where(half, a, pltpu.roll(b, ROWS, 1)).astype(jnp.bfloat16)
            final[2 * p + 1, :, at] = jnp.where(half, pltpu.roll(a, ROWS, 1), b).astype(jnp.bfloat16)
            return 0

        lax.fori_loop(0, CHIPS, spread, 0, unroll=4)
        return jnp.where(lane == 2 * p, first, jnp.where(lane == 2 * p + 1, second, kept))

    kept = lax.fori_loop(0, PAIRS, finish, jnp.zeros((PIECE, LANES), jnp.float32))
    scales[...] = kept.T[: 2 * PAIRS, :]

    pltpu.make_async_copy(others, others, row_sem.at[0]).wait()
    blocks = served.at[pl.ds(0, BANK - 1)]
    pltpu.make_async_copy(blocks, blocks, bank_sem.at[0]).wait()
    pltpu.make_async_copy(blocks, blocks, bank_sem.at[1]).wait()
    for p in range(PAIRS):
        pltpu.make_async_copy(send.at[p, pl.ds(0, ZERO - 1)], send.at[p, pl.ds(0, ZERO - 1)], send_sem.at[p]).wait()


def write_out(final, scales, served, gate, up, down, scale_gate, scale_up, scale_down, router, sems):
    copies = []
    for i, (to_final, to_scale) in enumerate(((gate, scale_gate), (up, scale_up), (down, scale_down))):
        at = pl.ds(i * HEADS, HEADS)
        copies.append(pltpu.make_async_copy(final.at[at], to_final, sems.at[2 * i]))
        copies.append(pltpu.make_async_copy(scales.at[at], to_scale, sems.at[2 * i + 1]))
    copies.append(pltpu.make_async_copy(served, router, sems.at[6]))
    for copy in copies:
        copy.start()
    for copy in copies:
        copy.wait()


def local(master_gate, master_up, master_down, router_weight, router_gain):
    gate = master_gate.reshape(HEADS * ROWS, COLS)
    up = master_up.reshape(HEADS * ROWS, COLS)
    down = jnp.transpose(master_down, (0, 2, 1)).reshape(HEADS * ROWS, COLS)
    router = router_weight.T
    gain = router_gain.reshape(1, ROWS)
    anywhere = pl.BlockSpec(memory_space=pl.ANY)
    vmem = pl.BlockSpec(memory_space=pltpu.VMEM)
    wide = CHIPS * LANES
    held = (
        jax.ShapeDtypeStruct((2 * PAIRS, PIECE, wide), jnp.bfloat16),
        jax.ShapeDtypeStruct((2 * PAIRS, PIECE), jnp.float32),
        jax.ShapeDtypeStruct((BANK, HEADS, wide), jnp.bfloat16),
    )
    final, scales, served = pl.pallas_call(
        exchange,
        out_shape=held,
        in_specs=[pl.BlockSpec(memory_space=pltpu.HBM)] * 5,
        out_specs=(vmem,) * 3,
        scratch_shapes=[
            pltpu.VMEM((PAIRS, LANES, COLS), jnp.float32),
            pltpu.VMEM((HEADS, ROWS), jnp.float32),
            pltpu.VMEM((1, ROWS), jnp.float32),
            pltpu.VMEM((PAIRS, ZERO, PIECE, LANES), jnp.bfloat16),
            pltpu.VMEM((PAIRS, ZERO, PIECE, LANES), jnp.bfloat16),
            pltpu.VMEM((HEADS, LANES), jnp.bfloat16),
            pltpu.VMEM((HEADS, LANES), jnp.bfloat16),
            pltpu.VMEM((HEADS, wide), jnp.bfloat16),
            pltpu.SemaphoreType.DMA((PAIRS,)),
            pltpu.SemaphoreType.DMA((PAIRS,)),
            pltpu.SemaphoreType.DMA((PAIRS,)),
            pltpu.SemaphoreType.DMA((PAIRS,)),
            pltpu.SemaphoreType.DMA((2,)),
            pltpu.SemaphoreType.DMA((2,)),
            pltpu.SemaphoreType.DMA((2,)),
            pltpu.SemaphoreType.DMA((2,)),
        ],
        compiler_params=pltpu.CompilerParams(
            collective_id=0, has_side_effects=True, vmem_limit_bytes=24 * 2**20
        ),
        name="exchange",
    )(*(pltpu.with_memory_space_constraint(a, pltpu.HBM) for a in (gate, up, down, router, gain)))
    piece = jax.ShapeDtypeStruct((HEADS, PIECE, wide), jnp.bfloat16)
    scale = jax.ShapeDtypeStruct((HEADS, PIECE), jnp.float32)
    outs = pl.pallas_call(
        write_out,
        out_shape=(piece, piece, piece, scale, scale, scale, held[2]),
        in_specs=[vmem] * 3,
        out_specs=(anywhere,) * 7,
        scratch_shapes=[pltpu.SemaphoreType.DMA((7,))],
        compiler_params=pltpu.CompilerParams(vmem_limit_bytes=8 * 2**20),
        name="write_out",
    )(final, scales, served)
    final_gate, final_up, final_down, scale_gate, scale_up, scale_down, router_out = outs
    serve_router = router_out.reshape(BANK * HEADS, wide).T
    return (
        jnp.transpose(final_gate, (0, 2, 1)), jnp.transpose(final_up, (0, 2, 1)), final_down,
        scale_gate, scale_up, scale_down, serve_router,
    )


def solution(mesh):
    in_specs = (
        P("bank", "zero", None),
        P("bank", "zero", None),
        P("bank", None, "zero"),
        P("zero", "bank"),
        P("zero"),
    )
    out_specs = (
        P("bank", None, "zero"),
        P("bank", None, "zero"),
        P("bank", "zero", None),
        P("bank", "zero"),
        P("bank", "zero"),
        P("bank", "zero"),
        P(),
    )
    return jax.shard_map(local, mesh=mesh, in_specs=in_specs, out_specs=out_specs, check_vma=False)
```

```python
import functools

import jax
import jax.numpy as jnp
from jax import lax
from jax.experimental import pallas as pl
from jax.experimental.pallas import tpu as pltpu
from jax.sharding import PartitionSpec as P

MESH = pl.DeviceIdType.MESH
ZERO, BANK = 32, 8
CHIPS = ZERO // 2
HEADS = 8
PAIRS = 12
ROWS, COLS, PIECE, LANES = 64, 1024, 32, 128


TURNS = (4, 3, 5, 2, 6, 1, 7, 0)


def interleave(recv, factor, half, final, first, second):
    def spread(k, _):
        a = recv[2 * k].astype(jnp.float32) * factor
        b = recv[2 * k + 1].astype(jnp.float32) * factor
        at = pl.ds(pl.multiple_of(k * LANES, LANES), LANES)
        final[first, :, at] = jnp.where(half, a, pltpu.roll(b, ROWS, 1)).astype(jnp.bfloat16)
        final[second, :, at] = jnp.where(half, pltpu.roll(a, ROWS, 1), b).astype(jnp.bfloat16)
        return 0

    lax.fori_loop(0, CHIPS, spread, 0, unroll=4)


def finish(recv, p, final, first, second, kept):
    lane = lax.broadcasted_iota(jnp.int32, (PIECE, LANES), 1)
    half = lane < ROWS

    def square(k, total):
        a = recv[2 * k].astype(jnp.float32)
        b = recv[2 * k + 1].astype(jnp.float32)
        return total + (a * a + b * b)

    total = lax.fori_loop(0, CHIPS, square, jnp.zeros((PIECE, LANES), jnp.float32), unroll=4)
    low = jnp.sqrt(jnp.sum(jnp.where(half, total, 0.0), axis=1, keepdims=True))
    high = jnp.sqrt(jnp.sum(jnp.where(half, 0.0, total), axis=1, keepdims=True))
    interleave(recv, 1.0 / jnp.where(half, low, high), half, final, first, second)
    return jnp.where(lane == 2 * p, low, jnp.where(lane == 2 * p + 1, high, kept))


def exchange(
    gate, up, down, router_hbm, gain_hbm,
    final, last, scales, served,
    held, router, gain, send, recv, mine, other, rows,
    load_sem, send_sem, recv_sem, own_sem, pair_sem, row_sem, bank_sem, small_sem,
):
    me, bank = lax.axis_index("zero"), lax.axis_index("bank")
    z, low = lax.div(me, 4), lax.rem(me, 4)
    x, core, chip = lax.div(low, 2), lax.rem(me, 2), lax.div(me, 2)
    planes = [lax.rem(z + dz, 8) for dz in TURNS]
    places = [(1 - x) * 2 + 1 - core, (1 - x) * 2 + core, x * 2 + 1 - core, low]
    sources = (gate, up, down)

    def load(p):
        source = sources[p // 4]
        return pltpu.make_async_copy(source.at[pl.ds((p % 4) * LANES, LANES)], held.at[p], load_sem.at[p])

    load(0).start()
    barrier = pltpu.get_barrier_semaphore()
    for turn, plane in enumerate(planes):
        for place in places[: 3 if TURNS[turn] == 0 else 4]:
            pl.semaphore_signal(barrier, inc=1, device_id={"zero": plane * 4 + place}, device_id_type=MESH)
    for step in range(1, BANK):
        pl.semaphore_signal(barrier, inc=1, device_id={"bank": lax.rem(bank + step, BANK)}, device_id_type=MESH)

    small = (
        pltpu.make_async_copy(router_hbm, router, small_sem.at[0]),
        pltpu.make_async_copy(gain_hbm, gain, small_sem.at[1]),
    )
    for copy in small:
        copy.start()
    for p in range(1, PAIRS):
        load(p).start()

    def landing(p):
        return last if isinstance(p, int) and p == PAIRS - 1 else recv.at[p]

    def prepare(p, turn):
        plane = planes[turn]
        at = pl.multiple_of(plane * LANES, LANES)
        turned = held[p, :, pl.ds(at, LANES)].T.astype(jnp.bfloat16)
        send[p, pl.ds(plane * 4, 4)] = turned.reshape(4, PIECE, LANES)

    def start(p, turn):
        for place in places:
            peer = planes[turn] * 4 + place
            if TURNS[turn] == 0 and place is low:
                pltpu.make_async_copy(send.at[p, me], landing(p).at[me], own_sem.at[p]).start()
            else:
                pltpu.make_async_remote_copy(
                    src_ref=send.at[p, peer], dst_ref=landing(p).at[me], send_sem=send_sem.at[p],
                    recv_sem=recv_sem.at[p], device_id={"zero": peer}, device_id_type=MESH,
                ).start()

    load(0).wait()
    prepare(0, 0)
    prepare(0, 1)
    pl.semaphore_wait(barrier, ZERO - 1 + BANK - 1)
    for turn in range(8):
        if turn + 2 < 8:
            prepare(0, turn + 2)
        start(0, turn)

    for copy in small:
        copy.wait()
    part = (router[...] * gain[...]).astype(jnp.bfloat16)
    mine[...] = jnp.concatenate([part, part], axis=1)
    to_pair = pltpu.make_async_remote_copy(
        src_ref=mine, dst_ref=other, send_sem=pair_sem.at[0], recv_sem=pair_sem.at[1],
        device_id={"zero": chip * 2 + 1 - core}, device_id_type=MESH,
    )

    def prepare_and_start(p):
        load_p = pltpu.make_async_copy(gate.at[pl.ds(0, LANES)], held.at[p], load_sem.at[p])
        load_p.wait()
        prepare(p, 0)
        for turn in range(8):
            if turn + 1 < 8:
                prepare(p, turn + 1)
            start(p, turn)

    prepare_and_start(1)
    to_pair.start()
    prepare_and_start(2)
    to_pair.wait()
    lower = lax.broadcasted_iota(jnp.int32, (HEADS, LANES), 1) < ROWS
    keep_mine = jnp.where(lower, 0, 1) == core
    at_chip = pl.ds(pl.multiple_of(chip * LANES, LANES), LANES)
    rows[:, at_chip] = jnp.where(
        keep_mine, mine[...].astype(jnp.float32), other[...].astype(jnp.float32)
    ).astype(jnp.bfloat16)

    def row_copy(step):
        return pltpu.make_async_remote_copy(
            src_ref=rows.at[:, at_chip], dst_ref=rows.at[:, at_chip], send_sem=row_sem.at[0],
            recv_sem=row_sem.at[1], device_id={"zero": lax.rem(chip + step, CHIPS) * 2 + core}, device_id_type=MESH,
        )

    prepare_and_start(3)
    for step in range(1, CHIPS):
        row_copy(step).start()

    def next_pair(p, _):
        prepare_and_start(p)
        return 0

    lax.fori_loop(4, PAIRS - 1, next_pair, 0)
    prepare_and_start(PAIRS - 1)

    others = rows.at[:, pl.ds(0, (CHIPS - 1) * LANES)]
    pltpu.make_async_copy(others, others, row_sem.at[1]).wait()

    def bank_copy(step):
        return pltpu.make_async_remote_copy(
            src_ref=rows, dst_ref=served.at[bank], send_sem=bank_sem.at[0],
            recv_sem=bank_sem.at[1], device_id={"bank": lax.rem(bank + step, BANK)}, device_id_type=MESH,
        )

    for step in range(1, BANK):
        bank_copy(step).start()
    served[bank] = rows[...]

    def arrive(p):
        pieces = landing(p)
        pltpu.make_async_copy(send.at[p, me], pieces.at[me], own_sem.at[p]).wait()
        arrived = pieces.at[pl.ds(0, ZERO - 1)]
        pltpu.make_async_copy(arrived, arrived, recv_sem.at[p]).wait()
        sent = send.at[p, pl.ds(0, ZERO - 1)]
        pltpu.make_async_copy(sent, sent, send_sem.at[p]).wait()

    def take(p, kept):
        arrive(p)
        return finish(recv.at[p], p, final, 2 * p, 2 * p + 1, kept)

    scales[...] = lax.fori_loop(0, PAIRS - 1, take, jnp.zeros((PIECE, LANES), jnp.float32))
    pltpu.make_async_copy(others, others, row_sem.at[0]).wait()
    blocks = served.at[pl.ds(0, BANK - 1)]
    pltpu.make_async_copy(blocks, blocks, bank_sem.at[0]).wait()
    pltpu.make_async_copy(blocks, blocks, bank_sem.at[1]).wait()
    arrive(PAIRS - 1)


def write_out(
    final, last, scales, served,
    gate, up, down, scale_gate, scale_up, scale_down, router,
    tail, turned, sems,
):
    copies = []

    def put(source, target):
        copy = pltpu.make_async_copy(source, target, sems.at[len(copies)])
        copy.start()
        copies.append(copy)

    put(final.at[pl.ds(0, 8)], gate)
    put(final.at[pl.ds(8, 8)], up)
    put(final.at[pl.ds(16, 6)], down.at[pl.ds(0, 6)])
    put(served, router)
    kept = finish(last, PAIRS - 1, tail, 0, 1, scales[...])
    put(tail, down.at[pl.ds(6, 2)])
    turned[...] = kept.T[: 2 * PAIRS, :]
    for i, target in enumerate((scale_gate, scale_up, scale_down)):
        put(turned.at[pl.ds(i * HEADS, HEADS)], target)
    for copy in copies:
        copy.wait()


def local(master_gate, master_up, master_down, router_weight, router_gain):
    gate = master_gate.reshape(HEADS * ROWS, COLS)
    up = master_up.reshape(HEADS * ROWS, COLS)
    down = jnp.transpose(master_down, (0, 2, 1)).reshape(HEADS * ROWS, COLS)
    router = router_weight.T
    gain = router_gain.reshape(1, ROWS)
    anywhere = pl.BlockSpec(memory_space=pl.ANY)
    vmem = pl.BlockSpec(memory_space=pltpu.VMEM)
    wide = CHIPS * LANES
    held = (
        jax.ShapeDtypeStruct((2 * PAIRS - 2, PIECE, wide), jnp.bfloat16),
        jax.ShapeDtypeStruct((ZERO, PIECE, LANES), jnp.bfloat16),
        jax.ShapeDtypeStruct((PIECE, LANES), jnp.float32),
        jax.ShapeDtypeStruct((BANK, HEADS, wide), jnp.bfloat16),
    )
    final, last, scales, served = pl.pallas_call(
        exchange,
        out_shape=held,
        in_specs=[pl.BlockSpec(memory_space=pltpu.HBM)] * 5,
        out_specs=(vmem,) * 4,
        scratch_shapes=[
            pltpu.VMEM((PAIRS, LANES, COLS), jnp.float32),
            pltpu.VMEM((HEADS, ROWS), jnp.float32),
            pltpu.VMEM((1, ROWS), jnp.float32),
            pltpu.VMEM((PAIRS, ZERO, PIECE, LANES), jnp.bfloat16),
            pltpu.VMEM((PAIRS - 1, ZERO, PIECE, LANES), jnp.bfloat16),
            pltpu.VMEM((HEADS, LANES), jnp.bfloat16),
            pltpu.VMEM((HEADS, LANES), jnp.bfloat16),
            pltpu.VMEM((HEADS, wide), jnp.bfloat16),
            pltpu.SemaphoreType.DMA((PAIRS,)),
            pltpu.SemaphoreType.DMA((PAIRS,)),
            pltpu.SemaphoreType.DMA((PAIRS,)),
            pltpu.SemaphoreType.DMA((PAIRS,)),
            pltpu.SemaphoreType.DMA((2,)),
            pltpu.SemaphoreType.DMA((2,)),
            pltpu.SemaphoreType.DMA((2,)),
            pltpu.SemaphoreType.DMA((2,)),
        ],
        compiler_params=pltpu.CompilerParams(
            collective_id=0, has_side_effects=True, vmem_limit_bytes=24 * 2**20
        ),
        name="exchange",
    )(*(pltpu.with_memory_space_constraint(a, pltpu.HBM) for a in (gate, up, down, router, gain)))
    piece = jax.ShapeDtypeStruct((HEADS, PIECE, wide), jnp.bfloat16)
    scale = jax.ShapeDtypeStruct((HEADS, PIECE), jnp.float32)
    outs = pl.pallas_call(
        write_out,
        out_shape=(piece, piece, piece, scale, scale, scale, held[3]),
        in_specs=[vmem] * 4,
        out_specs=(anywhere,) * 7,
        scratch_shapes=[
            pltpu.VMEM((2, PIECE, wide), jnp.bfloat16),
            pltpu.VMEM((2 * PAIRS, PIECE), jnp.float32),
            pltpu.SemaphoreType.DMA((8,)),
        ],
        compiler_params=pltpu.CompilerParams(vmem_limit_bytes=8 * 2**20),
        name="write_out",
    )(final, last, scales, served)
    final_gate, final_up, final_down, scale_gate, scale_up, scale_down, router_out = outs
    serve_router = router_out.reshape(BANK * HEADS, wide).T
    return (
        jnp.transpose(final_gate, (0, 2, 1)), jnp.transpose(final_up, (0, 2, 1)), final_down,
        scale_gate, scale_up, scale_down, serve_router,
    )


def solution(mesh):
    in_specs = (
        P("bank", "zero", None),
        P("bank", "zero", None),
        P("bank", None, "zero"),
        P("zero", "bank"),
        P("zero"),
    )
    out_specs = (
        P("bank", None, "zero"),
        P("bank", None, "zero"),
        P("bank", "zero", None),
        P("bank", "zero"),
        P("bank", "zero"),
        P("bank", "zero"),
        P(),
    )
    return jax.shard_map(local, mesh=mesh, in_specs=in_specs, out_specs=out_specs, check_vma=False)
```

```python
import functools

import jax
import jax.numpy as jnp
from jax import lax
from jax.experimental import pallas as pl
from jax.experimental.pallas import tpu as pltpu
from jax.sharding import PartitionSpec as P

MESH = pl.DeviceIdType.MESH
ZERO, BANK = 32, 8
CHIPS = ZERO // 2
HEADS = 8
PAIRS = 12
CHUNKS, EACH = 6, 2
ROWS, COLS, PIECE, LANES = 64, 1024, 32, 128


NEAR = (1, -1, 0)
TURNS = (4, 3, -3, 2, -2, 1, -1, 0)
EARLY = 2


def interleave(recv, i, factor, half, final, first, second):
    def spread(k, _):
        a = recv[2 * k, i].astype(jnp.float32) * factor
        b = recv[2 * k + 1, i].astype(jnp.float32) * factor
        at = pl.ds(pl.multiple_of(k * LANES, LANES), LANES)
        final[first, :, at] = jnp.where(half, a, pltpu.roll(b, ROWS, 1)).astype(jnp.bfloat16)
        final[second, :, at] = jnp.where(half, pltpu.roll(a, ROWS, 1), b).astype(jnp.bfloat16)
        return 0

    lax.fori_loop(0, CHIPS, spread, 0, unroll=16)


def finish(recv, i, p, final, first, second, kept):
    lane = lax.broadcasted_iota(jnp.int32, (PIECE, LANES), 1)
    half = lane < ROWS

    def square(k, total):
        a = recv[2 * k, i].astype(jnp.float32)
        b = recv[2 * k + 1, i].astype(jnp.float32)
        return total + (a * a + b * b)

    total = lax.fori_loop(0, CHIPS, square, jnp.zeros((PIECE, LANES), jnp.float32), unroll=16)
    low = jnp.sqrt(jnp.sum(jnp.where(half, total, 0.0), axis=1, keepdims=True))
    high = jnp.sqrt(jnp.sum(jnp.where(half, 0.0, total), axis=1, keepdims=True))
    interleave(recv, i, 1.0 / jnp.where(half, low, high), half, final, first, second)
    return jnp.where(lane == 2 * p, low, jnp.where(lane == 2 * p + 1, high, kept))


def exchange(
    gate, up, down, router_hbm, gain_hbm,
    final, last, scales, served,
    held, router, gain, send, recv, mine, other, column, beside, rows,
    load_sem, send_sem, recv_sem, pair_sem, column_sem, beside_sem, bank_sem, small_sem, news,
):
    me, bank = lax.axis_index("zero"), lax.axis_index("bank")
    z, low = lax.div(me, 4), lax.rem(me, 4)
    x, core = lax.div(low, 2), lax.rem(me, 2)
    places = [(1 - x) * 2 + 1 - core, (1 - x) * 2 + core, x * 2 + 1 - core, low]
    sources = (gate, up, down)

    down_first = jnp.where(lax.rem(z + 2, 8) < 4, 0, 1)
    way = 1 - 2 * down_first

    def plane(dz):
        return lax.rem(z + 8 + way * dz, 8)

    def load(c):
        source, size = sources[c // 2], EACH * LANES
        return pltpu.make_async_copy(source.at[pl.ds((c % 2) * size, size)], held.at[c], load_sem.at[c])

    load(0).start()
    barrier = pltpu.get_barrier_semaphore()
    greeted = 0
    for dz in NEAR:
        for place in places[:3] if dz == 0 else places[2:]:
            pl.semaphore_signal(barrier, inc=1, device_id={"zero": plane(dz) * 4 + place}, device_id_type=MESH)
            greeted += 1
    for step in range(1, BANK):
        pl.semaphore_signal(barrier, inc=1, device_id={"bank": lax.rem(bank + step, BANK)}, device_id_type=MESH)
        greeted += 1

    small = (
        pltpu.make_async_copy(router_hbm, router, small_sem.at[0]),
        pltpu.make_async_copy(gain_hbm, gain, small_sem.at[1]),
    )
    for copy in small:
        copy.start()
    for c in range(1, CHUNKS):
        load(c).start()

    def landing(c):
        return last if isinstance(c, int) and c == CHUNKS - 1 else recv.at[c]

    def prepare(c, dz):
        at = pl.multiple_of(plane(dz) * LANES, LANES)
        for i in range(EACH):
            turned = held[c, pl.ds(i * LANES, LANES), pl.ds(at, LANES)].T.astype(jnp.bfloat16)
            send[c, pl.ds(plane(dz) * 4, 4), i] = turned.reshape(4, PIECE, LANES)

    def start(c, dz, some=slice(None)):
        for place in places[some]:
            peer = plane(dz) * 4 + place
            if dz == 0 and place is low:
                pltpu.make_async_copy(send.at[c, me], landing(c).at[me], recv_sem.at[c]).start()
            else:
                pltpu.make_async_remote_copy(
                    src_ref=send.at[c, peer], dst_ref=landing(c).at[me], send_sem=send_sem.at[0],
                    recv_sem=recv_sem.at[c], device_id={"zero": peer}, device_id_type=MESH,
                ).start()

    def heard_of(dz):
        upward = down_first if dz < 0 else 1 - down_first
        return news.at[(1 - upward) * 4 + abs(dz) - 1]

    def pass_on(dz):
        side = 1 if dz > 0 else -1
        upward = down_first if side < 0 else 1 - down_first
        target = plane(-side) * 4 + low
        pl.semaphore_signal(
            news.at[(1 - upward) * 4 + abs(dz)], inc=1, device_id={"zero": target}, device_id_type=MESH
        )

    load(0).wait()
    for dz in NEAR:
        prepare(0, dz)
    to_pair = pltpu.make_async_remote_copy(
        src_ref=mine, dst_ref=other, send_sem=pair_sem.at[0], recv_sem=pair_sem.at[1],
        device_id={"zero": z * 4 + places[2]}, device_id_type=MESH,
    )

    pl.semaphore_wait(barrier, greeted)
    for side in (1, -1):
        pl.semaphore_signal(
            news.at[down_first * 4 if side < 0 else (1 - down_first) * 4],
            inc=1, device_id={"zero": plane(side) * 4 + low}, device_id_type=MESH,
        )
    for c in range(EARLY):
        if c > 0:
            load(c).wait()
            for dz in NEAR:
                prepare(c, dz)
        for dz in NEAR:
            start(c, dz, slice(None) if dz == 0 else slice(2, None))
    for copy in small:
        copy.wait()
    part = (router[...] * gain[...]).astype(jnp.bfloat16)
    mine[...] = jnp.concatenate([part, part], axis=1)
    to_pair.start()
    for dz in (1, -1, 2, -2, 3, -3, 4, -4):
        pl.semaphore_wait(heard_of(dz), 1)
        if abs(dz) < 4:
            pass_on(dz)
        for c in range(EARLY if dz != -4 else 0):
            if abs(dz) > 1:
                prepare(c, dz)
            start(c, dz, slice(None) if abs(dz) > 1 else slice(0, 2))

    to_pair.wait()
    lower = lax.broadcasted_iota(jnp.int32, (HEADS, LANES), 1) < ROWS
    keep_mine = jnp.where(lower, 0, 1) == core
    mine[...] = jnp.where(
        keep_mine, mine[...].astype(jnp.float32), other[...].astype(jnp.float32)
    ).astype(jnp.bfloat16)

    def column_copy(dz):
        return pltpu.make_async_remote_copy(
            src_ref=mine, dst_ref=column.at[dz // 2], send_sem=column_sem.at[0], recv_sem=column_sem.at[1],
            device_id={"zero": lax.rem(z + dz, 8) * 4 + low}, device_id_type=MESH,
        )

    @pl.when(core == 0)
    def _():
        column[0] = mine[...]
        for dz in (4, 2, 6):
            column_copy(dz).start()

    @pl.when(core == 1)
    def _():
        for dz in (3, 5, 1, 7):
            column_copy(dz).start()

    def column_wait(which):
        @pl.when(core == 0)
        def _():
            pltpu.make_async_copy(column.at[pl.ds(0, 3)], column.at[pl.ds(0, 3)], column_sem.at[which]).wait()

        @pl.when(core == 1)
        def _():
            pltpu.make_async_copy(column, column, column_sem.at[which]).wait()

    def beside_copy(i):
        return pltpu.make_async_remote_copy(
            src_ref=column, dst_ref=beside.at[i], send_sem=beside_sem.at[0], recv_sem=beside_sem.at[1],
            device_id={"zero": z * 4 + places[i]}, device_id_type=MESH,
        )

    def bank_copy(step):
        return pltpu.make_async_remote_copy(
            src_ref=rows, dst_ref=served.at[bank], send_sem=bank_sem.at[0],
            recv_sem=bank_sem.at[1], device_id={"bank": lax.rem(bank + step, BANK)}, device_id_type=MESH,
        )

    def prepare_and_start(c):
        size = EACH * LANES
        pltpu.make_async_copy(gate.at[pl.ds(0, size)], held.at[c], load_sem.at[c]).wait()
        prepare(c, TURNS[0])
        for turn, dz in enumerate(TURNS):
            if turn + 1 < len(TURNS):
                prepare(c, TURNS[turn + 1])
            start(c, dz)

    def arrive(c):
        pltpu.make_async_copy(landing(c), landing(c), recv_sem.at[c]).wait()

    def take(c, kept):
        arrive(c)
        for i in range(EACH):
            p = c * EACH + i
            kept = finish(recv.at[c], i, p, final, 2 * p, 2 * p + 1, kept)
        return kept

    def step(c, kept):
        prepare_and_start(c)
        return take(c - EARLY, kept)

    kept = lax.fori_loop(EARLY, 4, step, jnp.zeros((PIECE, LANES), jnp.float32))
    column_wait(1)
    for i in range(3):
        beside_copy(i).start()
    kept = step(4, kept)
    prepare_and_start(CHUNKS - 1)
    pltpu.make_async_copy(beside, beside, beside_sem.at[1]).wait()
    for i in range(4):
        side, parity = lax.div(places[i], 2), lax.rem(places[i], 2)
        for j in range(4):
            chip = lax.rem(z + 8 - 2 * j - parity, 8) * 2 + side
            at = pl.ds(pl.multiple_of(chip * LANES, LANES), LANES)
            rows[:, at] = column[j] if i == 3 else beside[i, j]
    for peer in range(1, BANK):
        bank_copy(peer).start()
    served[bank] = rows[...]

    scales[...] = lax.fori_loop(CHUNKS - 1 - EARLY, CHUNKS - 1, take, kept)
    column_wait(0)
    pltpu.make_async_copy(beside, beside, beside_sem.at[0]).wait()
    blocks = served.at[pl.ds(0, BANK - 1)]
    pltpu.make_async_copy(blocks, blocks, bank_sem.at[0]).wait()
    pltpu.make_async_copy(blocks, blocks, bank_sem.at[1]).wait()
    arrive(CHUNKS - 1)
    sent = send.at[:, pl.ds(0, ZERO - 1)]
    pltpu.make_async_copy(sent, sent, send_sem.at[0]).wait()


def write_out(
    final, last, scales, served,
    gate, up, down, scale_gate, scale_up, scale_down, router,
    tail, turned, sems,
):
    copies = []

    def put(source, target):
        copy = pltpu.make_async_copy(source, target, sems.at[len(copies)])
        copy.start()
        copies.append(copy)

    put(final.at[pl.ds(0, 8)], gate)
    put(final.at[pl.ds(8, 8)], up)
    put(final.at[pl.ds(16, 4)], down.at[pl.ds(0, 4)])
    put(served, router)
    kept = scales[...]
    for i in range(EACH):
        kept = finish(last, i, PAIRS - EACH + i, tail, 2 * i, 2 * i + 1, kept)
        put(tail.at[pl.ds(2 * i, 2)], down.at[pl.ds(4 + 2 * i, 2)])
    turned[...] = kept.T[: 2 * PAIRS, :]
    for i, target in enumerate((scale_gate, scale_up, scale_down)):
        put(turned.at[pl.ds(i * HEADS, HEADS)], target)
    for copy in copies:
        copy.wait()


def local(master_gate, master_up, master_down, router_weight, router_gain):
    gate = master_gate.reshape(HEADS * ROWS, COLS)
    up = master_up.reshape(HEADS * ROWS, COLS)
    down = jnp.transpose(master_down, (0, 2, 1)).reshape(HEADS * ROWS, COLS)
    router = router_weight.T
    gain = router_gain.reshape(1, ROWS)
    anywhere = pl.BlockSpec(memory_space=pl.ANY)
    vmem = pl.BlockSpec(memory_space=pltpu.VMEM)
    wide = CHIPS * LANES
    held = (
        jax.ShapeDtypeStruct((2 * (PAIRS - EACH), PIECE, wide), jnp.bfloat16),
        jax.ShapeDtypeStruct((ZERO, EACH, PIECE, LANES), jnp.bfloat16),
        jax.ShapeDtypeStruct((PIECE, LANES), jnp.float32),
        jax.ShapeDtypeStruct((BANK, HEADS, wide), jnp.bfloat16),
    )
    final, last, scales, served = pl.pallas_call(
        exchange,
        out_shape=held,
        in_specs=[pl.BlockSpec(memory_space=pltpu.HBM)] * 5,
        out_specs=(vmem,) * 4,
        scratch_shapes=[
            pltpu.VMEM((CHUNKS, EACH * LANES, COLS), jnp.float32),
            pltpu.VMEM((HEADS, ROWS), jnp.float32),
            pltpu.VMEM((1, ROWS), jnp.float32),
            pltpu.VMEM((CHUNKS, ZERO, EACH, PIECE, LANES), jnp.bfloat16),
            pltpu.VMEM((CHUNKS - 1, ZERO, EACH, PIECE, LANES), jnp.bfloat16),
            pltpu.VMEM((HEADS, LANES), jnp.bfloat16),
            pltpu.VMEM((HEADS, LANES), jnp.bfloat16),
            pltpu.VMEM((4, HEADS, LANES), jnp.bfloat16),
            pltpu.VMEM((3, 4, HEADS, LANES), jnp.bfloat16),
            pltpu.VMEM((HEADS, wide), jnp.bfloat16),
            pltpu.SemaphoreType.DMA((CHUNKS,)),
            pltpu.SemaphoreType.DMA((1,)),
            pltpu.SemaphoreType.DMA((CHUNKS,)),
            pltpu.SemaphoreType.DMA((2,)),
            pltpu.SemaphoreType.DMA((2,)),
            pltpu.SemaphoreType.DMA((2,)),
            pltpu.SemaphoreType.DMA((2,)),
            pltpu.SemaphoreType.DMA((2,)),
            pltpu.SemaphoreType.REGULAR((8,)),
        ],
        compiler_params=pltpu.CompilerParams(
            collective_id=0, has_side_effects=True, vmem_limit_bytes=24 * 2**20
        ),
        name="exchange",
    )(*(pltpu.with_memory_space_constraint(a, pltpu.HBM) for a in (gate, up, down, router, gain)))
    piece = jax.ShapeDtypeStruct((HEADS, PIECE, wide), jnp.bfloat16)
    scale = jax.ShapeDtypeStruct((HEADS, PIECE), jnp.float32)
    outs = pl.pallas_call(
        write_out,
        out_shape=(piece, piece, piece, scale, scale, scale, held[3]),
        in_specs=[vmem] * 4,
        out_specs=(anywhere,) * 7,
        scratch_shapes=[
            pltpu.VMEM((2 * EACH, PIECE, wide), jnp.bfloat16),
            pltpu.VMEM((2 * PAIRS, PIECE), jnp.float32),
            pltpu.SemaphoreType.DMA((9,)),
        ],
        compiler_params=pltpu.CompilerParams(vmem_limit_bytes=8 * 2**20),
        name="write_out",
    )(final, last, scales, served)
    final_gate, final_up, final_down, scale_gate, scale_up, scale_down, router_out = outs
    serve_router = router_out.reshape(BANK * HEADS, wide).T
    return (
        jnp.transpose(final_gate, (0, 2, 1)), jnp.transpose(final_up, (0, 2, 1)), final_down,
        scale_gate, scale_up, scale_down, serve_router,
    )


def solution(mesh):
    in_specs = (
        P("bank", "zero", None),
        P("bank", "zero", None),
        P("bank", None, "zero"),
        P("zero", "bank"),
        P("zero"),
    )
    out_specs = (
        P("bank", None, "zero"),
        P("bank", None, "zero"),
        P("bank", "zero", None),
        P("bank", "zero"),
        P("bank", "zero"),
        P("bank", "zero"),
        P(),
    )
    return jax.shard_map(local, mesh=mesh, in_specs=in_specs, out_specs=out_specs, check_vma=False)
```

```python
import functools

import jax
import jax.numpy as jnp
from jax import lax
from jax.experimental import pallas as pl
from jax.experimental.pallas import tpu as pltpu
from jax.sharding import PartitionSpec as P

MESH = pl.DeviceIdType.MESH
ZERO, BANK = 32, 8
CHIPS = ZERO // 2
HEADS = 8
PAIRS = 12
CHUNKS, EACH = 6, 2
ROWS, COLS, PIECE, LANES = 64, 1024, 32, 128


NEAR = (1, -1, 0)
TURNS = (4, 3, -3, 2, -2, 1, -1, 0)
EARLY = 2


def interleave(recv, i, factor, half, final, first, second):
    def spread(k, _):
        a = recv[2 * k, i].astype(jnp.float32) * factor
        b = recv[2 * k + 1, i].astype(jnp.float32) * factor
        at = pl.ds(pl.multiple_of(k * LANES, LANES), LANES)
        final[first, :, at] = jnp.where(half, a, pltpu.roll(b, ROWS, 1)).astype(jnp.bfloat16)
        final[second, :, at] = jnp.where(half, pltpu.roll(a, ROWS, 1), b).astype(jnp.bfloat16)
        return 0

    lax.fori_loop(0, CHIPS, spread, 0, unroll=16)


def finish(recv, i, p, final, first, second, kept):
    lane = lax.broadcasted_iota(jnp.int32, (PIECE, LANES), 1)
    half = lane < ROWS

    def square(k, total):
        a = recv[2 * k, i].astype(jnp.float32)
        b = recv[2 * k + 1, i].astype(jnp.float32)
        return total + (a * a + b * b)

    total = lax.fori_loop(0, CHIPS, square, jnp.zeros((PIECE, LANES), jnp.float32), unroll=16)
    low = jnp.sqrt(jnp.sum(jnp.where(half, total, 0.0), axis=1, keepdims=True))
    high = jnp.sqrt(jnp.sum(jnp.where(half, 0.0, total), axis=1, keepdims=True))
    interleave(recv, i, 1.0 / jnp.where(half, low, high), half, final, first, second)
    return jnp.where(lane == 2 * p, low, jnp.where(lane == 2 * p + 1, high, kept))


def exchange(
    gate, up, down, router_hbm, gain_hbm,
    final, last, scales, served,
    held, router, gain, send, recv, mine, other, column, beside, rows,
    load_sem, send_sem, recv_sem, pair_sem, column_sem, beside_sem, bank_sem, small_sem, news,
    block_sem, whole, everyone,
):
    me, bank = lax.axis_index("zero"), lax.axis_index("bank")
    z, low = lax.div(me, 4), lax.rem(me, 4)
    x, core = lax.div(low, 2), lax.rem(me, 2)
    places = [(1 - x) * 2 + 1 - core, (1 - x) * 2 + core, x * 2 + 1 - core, low]
    sources = (gate, up, down)

    down_first = jnp.where(lax.rem(z + 2, 8) < 4, 0, 1)
    way = 1 - 2 * down_first

    def plane(dz):
        return lax.rem(z + 8 + way * dz, 8)

    def load(c):
        source, size = sources[c // 2], EACH * LANES
        return pltpu.make_async_copy(source.at[pl.ds((c % 2) * size, size)], held.at[c], load_sem.at[c])

    def load_block(dz):
        at = pl.ds(pl.multiple_of(plane(dz) * LANES, LANES), LANES)
        return pltpu.make_async_copy(
            gate.at[pl.ds(0, EACH * LANES), at], held.at[0, :, at], block_sem.at[TURNS.index(dz)]
        )

    for dz in NEAR:
        load_block(dz).start()
    barrier = pltpu.get_barrier_semaphore()
    near = [(0, places[0]), (0, places[1]), (1, low), (-1, low), (1, places[2]), (-1, places[2]), (0, places[2])]
    for dz, place in near:
        pl.semaphore_signal(barrier, inc=1, device_id={"zero": plane(dz) * 4 + place}, device_id_type=MESH)

    def to_banks(signalled):
        for step in range(1, BANK):
            pl.semaphore_signal(
                signalled, inc=1, device_id={"bank": lax.rem(bank + step, BANK)}, device_id_type=MESH
            )

    @pl.when(z == 0)
    def _():
        to_banks(barrier)

    for dz in (2, -2, 3, -3, 4):
        load_block(dz).start()
    small = (
        pltpu.make_async_copy(router_hbm, router, small_sem.at[0]),
        pltpu.make_async_copy(gain_hbm, gain, small_sem.at[1]),
    )
    for copy in small:
        copy.start()
    for c in range(1, CHUNKS):
        load(c).start()

    def landing(c):
        return last if isinstance(c, int) and c == CHUNKS - 1 else recv.at[c]

    def prepare(c, dz):
        at = pl.multiple_of(plane(dz) * LANES, LANES)
        for i in range(EACH):
            turned = held[c, pl.ds(i * LANES, LANES), pl.ds(at, LANES)].T.astype(jnp.bfloat16)
            send[c, pl.ds(plane(dz) * 4, 4), i] = turned.reshape(4, PIECE, LANES)

    def start(c, dz, some=slice(None)):
        for place in places[some]:
            peer = plane(dz) * 4 + place
            if dz == 0 and place is low:
                pltpu.make_async_copy(send.at[c, me], landing(c).at[me], recv_sem.at[c]).start()
            else:
                pltpu.make_async_remote_copy(
                    src_ref=send.at[c, peer], dst_ref=landing(c).at[me], send_sem=send_sem.at[0],
                    recv_sem=recv_sem.at[c], device_id={"zero": peer}, device_id_type=MESH,
                ).start()

    def heard_of(dz):
        upward = down_first if dz < 0 else 1 - down_first
        return news.at[(1 - upward) * 4 + abs(dz) - 1]

    def pass_on(dz):
        side = 1 if dz > 0 else -1
        upward = down_first if side < 0 else 1 - down_first
        target = plane(-side) * 4 + low
        pl.semaphore_signal(
            news.at[(1 - upward) * 4 + abs(dz)], inc=1, device_id={"zero": target}, device_id_type=MESH
        )

    for dz in NEAR:
        load_block(dz).wait()
        prepare(0, dz)
    to_pair = pltpu.make_async_remote_copy(
        src_ref=mine, dst_ref=other, send_sem=pair_sem.at[0], recv_sem=pair_sem.at[1],
        device_id={"zero": z * 4 + places[2]}, device_id_type=MESH,
    )

    @pl.when(z == 0)
    def _():
        pl.semaphore_wait(barrier, len(near) + BANK - 1)

    @pl.when(z != 0)
    def _():
        pl.semaphore_wait(barrier, len(near))

    for side in (1, -1):
        pl.semaphore_signal(
            news.at[down_first * 4 if side < 0 else (1 - down_first) * 4],
            inc=1, device_id={"zero": plane(side) * 4 + low}, device_id_type=MESH,
        )
    for c in range(EARLY):
        if c > 0:
            load(c).wait()
            for dz in NEAR:
                prepare(c, dz)
        for dz in NEAR:
            start(c, dz, slice(None) if dz == 0 else slice(2, None))
    for copy in small:
        copy.wait()
    part = (router[...] * gain[...]).astype(jnp.bfloat16)
    mine[...] = jnp.concatenate([part, part], axis=1)
    to_pair.start()
    for dz in (1, -1, 2, -2, 3, -3, 4, -4):
        pl.semaphore_wait(heard_of(dz), 1)
        if abs(dz) < 4:
            pass_on(dz)
        if abs(dz) > 1 and dz != -4:
            load_block(dz).wait()
            for c in range(EARLY):
                prepare(c, dz)
        for c in range(EARLY if dz != -4 else 0):
            start(c, dz, slice(None) if abs(dz) > 1 else slice(0, 2))

    @pl.when(z == 0)
    def _():
        to_banks(whole)

    to_pair.wait()
    lower = lax.broadcasted_iota(jnp.int32, (HEADS, LANES), 1) < ROWS
    keep_mine = jnp.where(lower, 0, 1) == core
    mine[...] = jnp.where(
        keep_mine, mine[...].astype(jnp.float32), other[...].astype(jnp.float32)
    ).astype(jnp.bfloat16)

    def column_copy(dz):
        return pltpu.make_async_remote_copy(
            src_ref=mine, dst_ref=column.at[dz // 2], send_sem=column_sem.at[0], recv_sem=column_sem.at[1],
            device_id={"zero": lax.rem(z + dz, 8) * 4 + low}, device_id_type=MESH,
        )

    @pl.when(core == 0)
    def _():
        column[0] = mine[...]
        for dz in (4, 2, 6):
            column_copy(dz).start()

    @pl.when(core == 1)
    def _():
        for dz in (3, 5, 1, 7):
            column_copy(dz).start()

    def column_wait(which):
        @pl.when(core == 0)
        def _():
            pltpu.make_async_copy(column.at[pl.ds(0, 3)], column.at[pl.ds(0, 3)], column_sem.at[which]).wait()

        @pl.when(core == 1)
        def _():
            pltpu.make_async_copy(column, column, column_sem.at[which]).wait()

    def beside_copy(i):
        return pltpu.make_async_remote_copy(
            src_ref=column, dst_ref=beside.at[i], send_sem=beside_sem.at[0], recv_sem=beside_sem.at[1],
            device_id={"zero": z * 4 + places[i]}, device_id_type=MESH,
        )

    def bank_copy(step):
        return pltpu.make_async_remote_copy(
            src_ref=rows, dst_ref=served.at[bank], send_sem=bank_sem.at[0],
            recv_sem=bank_sem.at[1], device_id={"bank": lax.rem(bank + step, BANK)}, device_id_type=MESH,
        )

    def prepare_and_start(c):
        size = EACH * LANES
        pltpu.make_async_copy(gate.at[pl.ds(0, size)], held.at[c], load_sem.at[c]).wait()
        prepare(c, TURNS[0])
        for turn, dz in enumerate(TURNS):
            if turn + 1 < len(TURNS):
                prepare(c, TURNS[turn + 1])
            start(c, dz)

    def arrive(c):
        pltpu.make_async_copy(landing(c), landing(c), recv_sem.at[c]).wait()

    def take(c, kept):
        arrive(c)
        for i in range(EACH):
            p = c * EACH + i
            kept = finish(recv.at[c], i, p, final, 2 * p, 2 * p + 1, kept)
        return kept

    def step(c, kept):
        prepare_and_start(c)
        return take(c - EARLY, kept)

    kept = lax.fori_loop(EARLY, 4, step, jnp.zeros((PIECE, LANES), jnp.float32))
    @pl.when(z == 0)
    def _():
        pl.semaphore_wait(whole, BANK - 1)
        for other_z in range(1, 8):
            pl.semaphore_signal(everyone, inc=1, device_id={"zero": other_z * 4 + low}, device_id_type=MESH)

    column_wait(1)
    for i in range(3):
        beside_copy(i).start()
    kept = step(4, kept)
    prepare_and_start(CHUNKS - 1)
    pltpu.make_async_copy(beside, beside, beside_sem.at[1]).wait()
    for i in range(4):
        side, parity = lax.div(places[i], 2), lax.rem(places[i], 2)
        for j in range(4):
            chip = lax.rem(z + 8 - 2 * j - parity, 8) * 2 + side
            at = pl.ds(pl.multiple_of(chip * LANES, LANES), LANES)
            rows[:, at] = column[j] if i == 3 else beside[i, j]

    @pl.when(z != 0)
    def _():
        pl.semaphore_wait(everyone, 1)

    for peer in range(1, BANK):
        bank_copy(peer).start()
    served[bank] = rows[...]

    scales[...] = lax.fori_loop(CHUNKS - 1 - EARLY, CHUNKS - 1, take, kept)
    column_wait(0)
    pltpu.make_async_copy(beside, beside, beside_sem.at[0]).wait()
    blocks = served.at[pl.ds(0, BANK - 1)]
    pltpu.make_async_copy(blocks, blocks, bank_sem.at[0]).wait()
    pltpu.make_async_copy(blocks, blocks, bank_sem.at[1]).wait()
    arrive(CHUNKS - 1)
    sent = send.at[:, pl.ds(0, ZERO - 1)]
    pltpu.make_async_copy(sent, sent, send_sem.at[0]).wait()


def write_out(
    final, last, scales, served,
    gate, up, down, scale_gate, scale_up, scale_down, router,
    tail, turned, sems,
):
    copies = []

    def put(source, target):
        copy = pltpu.make_async_copy(source, target, sems.at[len(copies)])
        copy.start()
        copies.append(copy)

    put(final.at[pl.ds(0, 8)], gate)
    put(final.at[pl.ds(8, 8)], up)
    put(final.at[pl.ds(16, 4)], down.at[pl.ds(0, 4)])
    put(served, router)
    kept = scales[...]
    for i in range(EACH):
        kept = finish(last, i, PAIRS - EACH + i, tail, 2 * i, 2 * i + 1, kept)
        put(tail.at[pl.ds(2 * i, 2)], down.at[pl.ds(4 + 2 * i, 2)])
    turned[...] = kept.T[: 2 * PAIRS, :]
    for i, target in enumerate((scale_gate, scale_up, scale_down)):
        put(turned.at[pl.ds(i * HEADS, HEADS)], target)
    for copy in copies:
        copy.wait()


def local(master_gate, master_up, master_down, router_weight, router_gain):
    gate = master_gate.reshape(HEADS * ROWS, COLS)
    up = master_up.reshape(HEADS * ROWS, COLS)
    down = jnp.transpose(master_down, (0, 2, 1)).reshape(HEADS * ROWS, COLS)
    router = router_weight.T
    gain = router_gain.reshape(1, ROWS)
    anywhere = pl.BlockSpec(memory_space=pl.ANY)
    vmem = pl.BlockSpec(memory_space=pltpu.VMEM)
    wide = CHIPS * LANES
    held = (
        jax.ShapeDtypeStruct((2 * (PAIRS - EACH), PIECE, wide), jnp.bfloat16),
        jax.ShapeDtypeStruct((ZERO, EACH, PIECE, LANES), jnp.bfloat16),
        jax.ShapeDtypeStruct((PIECE, LANES), jnp.float32),
        jax.ShapeDtypeStruct((BANK, HEADS, wide), jnp.bfloat16),
    )
    final, last, scales, served = pl.pallas_call(
        exchange,
        out_shape=held,
        in_specs=[pl.BlockSpec(memory_space=pltpu.HBM)] * 5,
        out_specs=(vmem,) * 4,
        scratch_shapes=[
            pltpu.VMEM((CHUNKS, EACH * LANES, COLS), jnp.float32),
            pltpu.VMEM((HEADS, ROWS), jnp.float32),
            pltpu.VMEM((1, ROWS), jnp.float32),
            pltpu.VMEM((CHUNKS, ZERO, EACH, PIECE, LANES), jnp.bfloat16),
            pltpu.VMEM((CHUNKS - 1, ZERO, EACH, PIECE, LANES), jnp.bfloat16),
            pltpu.VMEM((HEADS, LANES), jnp.bfloat16),
            pltpu.VMEM((HEADS, LANES), jnp.bfloat16),
            pltpu.VMEM((4, HEADS, LANES), jnp.bfloat16),
            pltpu.VMEM((3, 4, HEADS, LANES), jnp.bfloat16),
            pltpu.VMEM((HEADS, wide), jnp.bfloat16),
            pltpu.SemaphoreType.DMA((CHUNKS,)),
            pltpu.SemaphoreType.DMA((1,)),
            pltpu.SemaphoreType.DMA((CHUNKS,)),
            pltpu.SemaphoreType.DMA((2,)),
            pltpu.SemaphoreType.DMA((2,)),
            pltpu.SemaphoreType.DMA((2,)),
            pltpu.SemaphoreType.DMA((2,)),
            pltpu.SemaphoreType.DMA((2,)),
            pltpu.SemaphoreType.REGULAR((8,)),
            pltpu.SemaphoreType.DMA((8,)),
            pltpu.SemaphoreType.REGULAR,
            pltpu.SemaphoreType.REGULAR,
        ],
        compiler_params=pltpu.CompilerParams(
            collective_id=0, has_side_effects=True, vmem_limit_bytes=24 * 2**20
        ),
        name="exchange",
    )(*(pltpu.with_memory_space_constraint(a, pltpu.HBM) for a in (gate, up, down, router, gain)))
    piece = jax.ShapeDtypeStruct((HEADS, PIECE, wide), jnp.bfloat16)
    scale = jax.ShapeDtypeStruct((HEADS, PIECE), jnp.float32)
    outs = pl.pallas_call(
        write_out,
        out_shape=(piece, piece, piece, scale, scale, scale, held[3]),
        in_specs=[vmem] * 4,
        out_specs=(anywhere,) * 7,
        scratch_shapes=[
            pltpu.VMEM((2 * EACH, PIECE, wide), jnp.bfloat16),
            pltpu.VMEM((2 * PAIRS, PIECE), jnp.float32),
            pltpu.SemaphoreType.DMA((9,)),
        ],
        compiler_params=pltpu.CompilerParams(vmem_limit_bytes=8 * 2**20),
        name="write_out",
    )(final, last, scales, served)
    final_gate, final_up, final_down, scale_gate, scale_up, scale_down, router_out = outs
    serve_router = router_out.reshape(BANK * HEADS, wide).T
    return (
        jnp.transpose(final_gate, (0, 2, 1)), jnp.transpose(final_up, (0, 2, 1)), final_down,
        scale_gate, scale_up, scale_down, serve_router,
    )


def solution(mesh):
    in_specs = (
        P("bank", "zero", None),
        P("bank", "zero", None),
        P("bank", None, "zero"),
        P("zero", "bank"),
        P("zero"),
    )
    out_specs = (
        P("bank", None, "zero"),
        P("bank", None, "zero"),
        P("bank", "zero", None),
        P("bank", "zero"),
        P("bank", "zero"),
        P("bank", "zero"),
        P(),
    )
    return jax.shard_map(local, mesh=mesh, in_specs=in_specs, out_specs=out_specs, check_vma=False)
```

```python
import functools

import jax
import jax.numpy as jnp
from jax import lax
from jax.experimental import pallas as pl
from jax.experimental.pallas import tpu as pltpu
from jax.sharding import PartitionSpec as P

MESH = pl.DeviceIdType.MESH
ZERO, BANK = 32, 8
CHIPS = ZERO // 2
HEADS = 8
PAIRS = 12
CHUNKS, EACH = 6, 2
ROWS, COLS, PIECE, LANES = 64, 1024, 32, 128


NEAR = (1, -1, 0)
TURNS = (4, 3, -3, 2, -2, 1, -1, 0)
EARLY = 3


def interleave(recv, i, factor, half, final, first, second):
    def spread(k, _):
        a = recv[2 * k, i].astype(jnp.float32) * factor
        b = recv[2 * k + 1, i].astype(jnp.float32) * factor
        at = pl.ds(pl.multiple_of(k * LANES, LANES), LANES)
        final[first, :, at] = jnp.where(half, a, pltpu.roll(b, ROWS, 1)).astype(jnp.bfloat16)
        final[second, :, at] = jnp.where(half, pltpu.roll(a, ROWS, 1), b).astype(jnp.bfloat16)
        return 0

    lax.fori_loop(0, CHIPS, spread, 0, unroll=16)


def finish(recv, i, p, final, first, second, kept):
    lane = lax.broadcasted_iota(jnp.int32, (PIECE, LANES), 1)
    half = lane < ROWS

    def square(k, total):
        a = recv[2 * k, i].astype(jnp.float32)
        b = recv[2 * k + 1, i].astype(jnp.float32)
        return total + (a * a + b * b)

    total = lax.fori_loop(0, CHIPS, square, jnp.zeros((PIECE, LANES), jnp.float32), unroll=16)
    low = jnp.sqrt(jnp.sum(jnp.where(half, total, 0.0), axis=1, keepdims=True))
    high = jnp.sqrt(jnp.sum(jnp.where(half, 0.0, total), axis=1, keepdims=True))
    interleave(recv, i, 1.0 / jnp.where(half, low, high), half, final, first, second)
    return jnp.where(lane == 2 * p, low, jnp.where(lane == 2 * p + 1, high, kept))


def exchange(
    gate, up, down, router_hbm, gain_hbm,
    final, last, scales, served,
    held, router, gain, send, recv, mine, other, column, beside, rows,
    load_sem, send_sem, recv_sem, pair_sem, column_sem, beside_sem, bank_sem, small_sem, news,
    block_sem, whole, everyone,
):
    me, bank = lax.axis_index("zero"), lax.axis_index("bank")
    z, low = lax.div(me, 4), lax.rem(me, 4)
    x, core = lax.div(low, 2), lax.rem(me, 2)
    places = [(1 - x) * 2 + 1 - core, (1 - x) * 2 + core, x * 2 + 1 - core, low]
    sources = (gate, up, down)

    down_first = jnp.where(lax.rem(z + 2, 8) < 4, 0, 1)
    way = 1 - 2 * down_first

    def plane(dz):
        return lax.rem(z + 8 + way * dz, 8)

    def load(c):
        source, size = sources[c // 2], EACH * LANES
        return pltpu.make_async_copy(source.at[pl.ds((c % 2) * size, size)], held.at[c], load_sem.at[c])

    def load_block(dz):
        at = pl.ds(pl.multiple_of(plane(dz) * LANES, LANES), LANES)
        return pltpu.make_async_copy(
            gate.at[pl.ds(0, EACH * LANES), at], held.at[0, :, at], block_sem.at[TURNS.index(dz)]
        )

    for dz in NEAR:
        load_block(dz).start()
    barrier = pltpu.get_barrier_semaphore()
    near = [(0, places[0]), (0, places[1]), (1, low), (-1, low), (1, places[2]), (-1, places[2]), (0, places[2])]
    for dz, place in near:
        pl.semaphore_signal(barrier, inc=1, device_id={"zero": plane(dz) * 4 + place}, device_id_type=MESH)

    def to_banks(signalled):
        for step in range(1, BANK):
            pl.semaphore_signal(
                signalled, inc=1, device_id={"bank": lax.rem(bank + step, BANK)}, device_id_type=MESH
            )

    @pl.when(z == 0)
    def _():
        to_banks(barrier)

    for dz in (2, -2, 3, -3, 4):
        load_block(dz).start()
    small = (
        pltpu.make_async_copy(router_hbm, router, small_sem.at[0]),
        pltpu.make_async_copy(gain_hbm, gain, small_sem.at[1]),
    )
    for copy in small:
        copy.start()
    for c in range(1, CHUNKS):
        load(c).start()

    def landing(c):
        return last if isinstance(c, int) and c == CHUNKS - 1 else recv.at[c]

    def prepare(c, dz):
        at = pl.multiple_of(plane(dz) * LANES, LANES)
        for i in range(EACH):
            turned = held[c, pl.ds(i * LANES, LANES), pl.ds(at, LANES)].T.astype(jnp.bfloat16)
            send[c, pl.ds(plane(dz) * 4, 4), i] = turned.reshape(4, PIECE, LANES)

    def start(c, dz, some=slice(None)):
        for place in places[some]:
            peer = plane(dz) * 4 + place
            if dz == 0 and place is low:
                pltpu.make_async_copy(send.at[c, me], landing(c).at[me], recv_sem.at[c]).start()
            else:
                pltpu.make_async_remote_copy(
                    src_ref=send.at[c, peer], dst_ref=landing(c).at[me], send_sem=send_sem.at[0],
                    recv_sem=recv_sem.at[c], device_id={"zero": peer}, device_id_type=MESH,
                ).start()

    def heard_of(dz):
        upward = down_first if dz < 0 else 1 - down_first
        return news.at[(1 - upward) * 4 + abs(dz) - 1]

    def pass_on(dz):
        side = 1 if dz > 0 else -1
        upward = down_first if side < 0 else 1 - down_first
        target = plane(-side) * 4 + low
        pl.semaphore_signal(
            news.at[(1 - upward) * 4 + abs(dz)], inc=1, device_id={"zero": target}, device_id_type=MESH
        )

    for dz in NEAR[:2]:
        load_block(dz).wait()
        prepare(0, dz)
    to_pair = pltpu.make_async_remote_copy(
        src_ref=mine, dst_ref=other, send_sem=pair_sem.at[0], recv_sem=pair_sem.at[1],
        device_id={"zero": z * 4 + places[2]}, device_id_type=MESH,
    )

    @pl.when(z == 0)
    def _():
        pl.semaphore_wait(barrier, len(near) + BANK - 1)

    @pl.when(z != 0)
    def _():
        pl.semaphore_wait(barrier, len(near))

    for side in (1, -1):
        pl.semaphore_signal(
            news.at[down_first * 4 if side < 0 else (1 - down_first) * 4],
            inc=1, device_id={"zero": plane(side) * 4 + low}, device_id_type=MESH,
        )
    for c in range(EARLY):
        if c > 0:
            load(c).wait()
            for dz in NEAR:
                prepare(c, dz)
        for dz in NEAR:
            if c == 0 and dz == 0:
                load_block(dz).wait()
                prepare(c, dz)
            start(c, dz, slice(None) if dz == 0 else slice(2, None))
    for copy in small:
        copy.wait()
    part = (router[...] * gain[...]).astype(jnp.bfloat16)
    mine[...] = jnp.concatenate([part, part], axis=1)
    to_pair.start()
    for dz in (1, -1, 2, -2, 3, -3, 4, -4):
        pl.semaphore_wait(heard_of(dz), 1)
        if abs(dz) < 4:
            pass_on(dz)
        if abs(dz) > 1 and dz != -4:
            load_block(dz).wait()
            for c in range(EARLY):
                prepare(c, dz)
        for c in range(EARLY if dz != -4 else 0):
            start(c, dz, slice(None) if abs(dz) > 1 else slice(0, 2))

    @pl.when(z == 0)
    def _():
        to_banks(whole)

    to_pair.wait()
    lower = lax.broadcasted_iota(jnp.int32, (HEADS, LANES), 1) < ROWS
    keep_mine = jnp.where(lower, 0, 1) == core
    mine[...] = jnp.where(
        keep_mine, mine[...].astype(jnp.float32), other[...].astype(jnp.float32)
    ).astype(jnp.bfloat16)

    def column_copy(dz):
        return pltpu.make_async_remote_copy(
            src_ref=mine, dst_ref=column.at[dz // 2], send_sem=column_sem.at[0], recv_sem=column_sem.at[1],
            device_id={"zero": lax.rem(z + dz, 8) * 4 + low}, device_id_type=MESH,
        )

    @pl.when(core == 0)
    def _():
        column[0] = mine[...]
        for dz in (4, 2, 6):
            column_copy(dz).start()

    @pl.when(core == 1)
    def _():
        for dz in (3, 5, 1, 7):
            column_copy(dz).start()

    def column_wait(which):
        @pl.when(core == 0)
        def _():
            pltpu.make_async_copy(column.at[pl.ds(0, 3)], column.at[pl.ds(0, 3)], column_sem.at[which]).wait()

        @pl.when(core == 1)
        def _():
            pltpu.make_async_copy(column, column, column_sem.at[which]).wait()

    def beside_copy(i):
        return pltpu.make_async_remote_copy(
            src_ref=column, dst_ref=beside.at[i], send_sem=beside_sem.at[0], recv_sem=beside_sem.at[1],
            device_id={"zero": z * 4 + places[i]}, device_id_type=MESH,
        )

    def bank_copy(step):
        return pltpu.make_async_remote_copy(
            src_ref=rows, dst_ref=served.at[bank], send_sem=bank_sem.at[0],
            recv_sem=bank_sem.at[1], device_id={"bank": lax.rem(bank + step, BANK)}, device_id_type=MESH,
        )

    def prepare_and_start(c):
        size = EACH * LANES
        pltpu.make_async_copy(gate.at[pl.ds(0, size)], held.at[c], load_sem.at[c]).wait()
        prepare(c, TURNS[0])
        for turn, dz in enumerate(TURNS):
            if turn + 1 < len(TURNS):
                prepare(c, TURNS[turn + 1])
            start(c, dz)

    def arrive(c):
        pltpu.make_async_copy(landing(c), landing(c), recv_sem.at[c]).wait()

    def take(c, kept):
        arrive(c)
        for i in range(EACH):
            p = c * EACH + i
            kept = finish(recv.at[c], i, p, final, 2 * p, 2 * p + 1, kept)
        return kept

    def step(c, kept):
        prepare_and_start(c)
        return take(c - EARLY, kept)

    kept = lax.fori_loop(EARLY, 4, step, jnp.zeros((PIECE, LANES), jnp.float32))
    @pl.when(z == 0)
    def _():
        pl.semaphore_wait(whole, BANK - 1)
        for other_z in range(1, 8):
            pl.semaphore_signal(everyone, inc=1, device_id={"zero": other_z * 4 + low}, device_id_type=MESH)

    column_wait(1)
    for i in range(3):
        beside_copy(i).start()
    kept = step(4, kept)
    prepare_and_start(CHUNKS - 1)
    pltpu.make_async_copy(beside, beside, beside_sem.at[1]).wait()
    for i in range(4):
        side, parity = lax.div(places[i], 2), lax.rem(places[i], 2)
        for j in range(4):
            chip = lax.rem(z + 8 - 2 * j - parity, 8) * 2 + side
            at = pl.ds(pl.multiple_of(chip * LANES, LANES), LANES)
            rows[:, at] = column[j] if i == 3 else beside[i, j]

    @pl.when(z != 0)
    def _():
        pl.semaphore_wait(everyone, 1)

    for peer in range(1, BANK):
        bank_copy(peer).start()
    served[bank] = rows[...]

    scales[...] = lax.fori_loop(CHUNKS - 1 - EARLY, CHUNKS - 1, take, kept)
    column_wait(0)
    pltpu.make_async_copy(beside, beside, beside_sem.at[0]).wait()
    blocks = served.at[pl.ds(0, BANK - 1)]
    pltpu.make_async_copy(blocks, blocks, bank_sem.at[0]).wait()
    pltpu.make_async_copy(blocks, blocks, bank_sem.at[1]).wait()
    arrive(CHUNKS - 1)
    sent = send.at[:, pl.ds(0, ZERO - 1)]
    pltpu.make_async_copy(sent, sent, send_sem.at[0]).wait()


def write_out(
    final, last, scales, served,
    gate, up, down, scale_gate, scale_up, scale_down, router,
    tail, turned, sems,
):
    copies = []

    def put(source, target):
        copy = pltpu.make_async_copy(source, target, sems.at[len(copies)])
        copy.start()
        copies.append(copy)

    put(final.at[pl.ds(0, 8)], gate)
    put(final.at[pl.ds(8, 8)], up)
    put(final.at[pl.ds(16, 4)], down.at[pl.ds(0, 4)])
    put(served, router)
    kept = scales[...]
    for i in range(EACH):
        kept = finish(last, i, PAIRS - EACH + i, tail, 2 * i, 2 * i + 1, kept)
        put(tail.at[pl.ds(2 * i, 2)], down.at[pl.ds(4 + 2 * i, 2)])
    turned[...] = kept.T[: 2 * PAIRS, :]
    for i, target in enumerate((scale_gate, scale_up, scale_down)):
        put(turned.at[pl.ds(i * HEADS, HEADS)], target)
    for copy in copies:
        copy.wait()


def local(master_gate, master_up, master_down, router_weight, router_gain):
    gate = master_gate.reshape(HEADS * ROWS, COLS)
    up = master_up.reshape(HEADS * ROWS, COLS)
    down = jnp.transpose(master_down, (0, 2, 1)).reshape(HEADS * ROWS, COLS)
    router = router_weight.T
    gain = router_gain.reshape(1, ROWS)
    anywhere = pl.BlockSpec(memory_space=pl.ANY)
    vmem = pl.BlockSpec(memory_space=pltpu.VMEM)
    wide = CHIPS * LANES
    held = (
        jax.ShapeDtypeStruct((2 * (PAIRS - EACH), PIECE, wide), jnp.bfloat16),
        jax.ShapeDtypeStruct((ZERO, EACH, PIECE, LANES), jnp.bfloat16),
        jax.ShapeDtypeStruct((PIECE, LANES), jnp.float32),
        jax.ShapeDtypeStruct((BANK, HEADS, wide), jnp.bfloat16),
    )
    final, last, scales, served = pl.pallas_call(
        exchange,
        out_shape=held,
        in_specs=[pl.BlockSpec(memory_space=pltpu.HBM)] * 5,
        out_specs=(vmem,) * 4,
        scratch_shapes=[
            pltpu.VMEM((CHUNKS, EACH * LANES, COLS), jnp.float32),
            pltpu.VMEM((HEADS, ROWS), jnp.float32),
            pltpu.VMEM((1, ROWS), jnp.float32),
            pltpu.VMEM((CHUNKS, ZERO, EACH, PIECE, LANES), jnp.bfloat16),
            pltpu.VMEM((CHUNKS - 1, ZERO, EACH, PIECE, LANES), jnp.bfloat16),
            pltpu.VMEM((HEADS, LANES), jnp.bfloat16),
            pltpu.VMEM((HEADS, LANES), jnp.bfloat16),
            pltpu.VMEM((4, HEADS, LANES), jnp.bfloat16),
            pltpu.VMEM((3, 4, HEADS, LANES), jnp.bfloat16),
            pltpu.VMEM((HEADS, wide), jnp.bfloat16),
            pltpu.SemaphoreType.DMA((CHUNKS,)),
            pltpu.SemaphoreType.DMA((1,)),
            pltpu.SemaphoreType.DMA((CHUNKS,)),
            pltpu.SemaphoreType.DMA((2,)),
            pltpu.SemaphoreType.DMA((2,)),
            pltpu.SemaphoreType.DMA((2,)),
            pltpu.SemaphoreType.DMA((2,)),
            pltpu.SemaphoreType.DMA((2,)),
            pltpu.SemaphoreType.REGULAR((8,)),
            pltpu.SemaphoreType.DMA((8,)),
            pltpu.SemaphoreType.REGULAR,
            pltpu.SemaphoreType.REGULAR,
        ],
        compiler_params=pltpu.CompilerParams(
            collective_id=0, has_side_effects=True, vmem_limit_bytes=24 * 2**20
        ),
        name="exchange",
    )(*(pltpu.with_memory_space_constraint(a, pltpu.HBM) for a in (gate, up, down, router, gain)))
    piece = jax.ShapeDtypeStruct((HEADS, PIECE, wide), jnp.bfloat16)
    scale = jax.ShapeDtypeStruct((HEADS, PIECE), jnp.float32)
    outs = pl.pallas_call(
        write_out,
        out_shape=(piece, piece, piece, scale, scale, scale, held[3]),
        in_specs=[vmem] * 4,
        out_specs=(anywhere,) * 7,
        scratch_shapes=[
            pltpu.VMEM((2 * EACH, PIECE, wide), jnp.bfloat16),
            pltpu.VMEM((2 * PAIRS, PIECE), jnp.float32),
            pltpu.SemaphoreType.DMA((9,)),
        ],
        compiler_params=pltpu.CompilerParams(vmem_limit_bytes=8 * 2**20),
        name="write_out",
    )(final, last, scales, served)
    final_gate, final_up, final_down, scale_gate, scale_up, scale_down, router_out = outs
    serve_router = router_out.reshape(BANK * HEADS, wide).T
    return (
        jnp.transpose(final_gate, (0, 2, 1)), jnp.transpose(final_up, (0, 2, 1)), final_down,
        scale_gate, scale_up, scale_down, serve_router,
    )


def solution(mesh):
    in_specs = (
        P("bank", "zero", None),
        P("bank", "zero", None),
        P("bank", None, "zero"),
        P("zero", "bank"),
        P("zero"),
    )
    out_specs = (
        P("bank", None, "zero"),
        P("bank", None, "zero"),
        P("bank", "zero", None),
        P("bank", "zero"),
        P("bank", "zero"),
        P("bank", "zero"),
        P(),
    )
    return jax.shard_map(local, mesh=mesh, in_specs=in_specs, out_specs=out_specs, check_vma=False)
```

```python
import functools

import jax
import jax.numpy as jnp
from jax import lax
from jax.experimental import pallas as pl
from jax.experimental.pallas import tpu as pltpu
from jax.sharding import PartitionSpec as P

MESH = pl.DeviceIdType.MESH
ZERO, BANK = 32, 8
CHIPS = ZERO // 2
HEADS = 8
PAIRS = 12
CHUNKS, EACH = 6, 2
ROWS, COLS, PIECE, LANES = 64, 1024, 32, 128


NEAR = (1, -1, 0)
TURNS = (4, 3, -3, 2, -2, 1, -1, 0)
EARLY = 3


def interleave(recv, i, factor, half, final, first, second):
    def spread(k, _):
        a = recv[2 * k, i].astype(jnp.float32) * factor
        b = recv[2 * k + 1, i].astype(jnp.float32) * factor
        at = pl.ds(pl.multiple_of(k * LANES, LANES), LANES)
        final[first, :, at] = jnp.where(half, a, pltpu.roll(b, ROWS, 1)).astype(jnp.bfloat16)
        final[second, :, at] = jnp.where(half, pltpu.roll(a, ROWS, 1), b).astype(jnp.bfloat16)
        return 0

    lax.fori_loop(0, CHIPS, spread, 0, unroll=16)


def finish(recv, i, p, final, first, second, kept):
    lane = lax.broadcasted_iota(jnp.int32, (PIECE, LANES), 1)
    half = lane < ROWS

    def square(k, total):
        a = recv[2 * k, i].astype(jnp.float32)
        b = recv[2 * k + 1, i].astype(jnp.float32)
        return total + (a * a + b * b)

    total = lax.fori_loop(0, CHIPS, square, jnp.zeros((PIECE, LANES), jnp.float32), unroll=16)
    low = jnp.sqrt(jnp.sum(jnp.where(half, total, 0.0), axis=1, keepdims=True))
    high = jnp.sqrt(jnp.sum(jnp.where(half, 0.0, total), axis=1, keepdims=True))
    interleave(recv, i, 1.0 / jnp.where(half, low, high), half, final, first, second)
    return jnp.where(lane == 2 * p, low, jnp.where(lane == 2 * p + 1, high, kept))


def exchange(
    gate, up, down, router_hbm, gain_hbm,
    final, last, scales, served,
    held, router, gain, send, recv, mine, other, column, beside, rows,
    load_sem, send_sem, recv_sem, pair_sem, column_sem, beside_sem, bank_sem, small_sem, news,
    block_sem, whole, everyone,
):
    me, bank = lax.axis_index("zero"), lax.axis_index("bank")
    z, low = lax.div(me, 4), lax.rem(me, 4)
    x, core = lax.div(low, 2), lax.rem(me, 2)
    places = [(1 - x) * 2 + 1 - core, (1 - x) * 2 + core, x * 2 + 1 - core, low]
    sources = (gate, up, down)

    down_first = jnp.where(lax.rem(z + 2, 8) < 4, 0, 1)
    way = 1 - 2 * down_first

    def plane(dz):
        return lax.rem(z + 8 + way * dz, 8)

    def load(c):
        source, size = sources[c // 2], EACH * LANES
        return pltpu.make_async_copy(source.at[pl.ds((c % 2) * size, size)], held.at[c], load_sem.at[c])

    def load_block(dz):
        at = pl.ds(pl.multiple_of(plane(dz) * LANES, LANES), LANES)
        return pltpu.make_async_copy(
            gate.at[pl.ds(0, EACH * LANES), at], held.at[0, :, at], block_sem.at[min(abs(dz) + 1, 3) % 3]
        )

    for dz in NEAR:
        load_block(dz).start()
    barrier = pltpu.get_barrier_semaphore()
    near = [(0, places[0]), (0, places[1]), (1, low), (-1, low), (1, places[2]), (-1, places[2]), (0, places[2])]
    for dz, place in near:
        pl.semaphore_signal(barrier, inc=1, device_id={"zero": plane(dz) * 4 + place}, device_id_type=MESH)

    def to_banks(signalled):
        for step in range(1, BANK):
            pl.semaphore_signal(
                signalled, inc=1, device_id={"bank": lax.rem(bank + step, BANK)}, device_id_type=MESH
            )

    @pl.when(z == 0)
    def _():
        to_banks(barrier)

    for dz in (2, -2, 3, -3, 4):
        load_block(dz).start()
    small = (
        pltpu.make_async_copy(router_hbm, router, small_sem.at[0]),
        pltpu.make_async_copy(gain_hbm, gain, small_sem.at[1]),
    )
    for copy in small:
        copy.start()
    for c in range(1, CHUNKS):
        load(c).start()

    def landing(c):
        return last if isinstance(c, int) and c == CHUNKS - 1 else recv.at[c]

    def prepare(c, dz):
        at = pl.multiple_of(plane(dz) * LANES, LANES)
        for i in range(EACH):
            turned = held[c, pl.ds(i * LANES, LANES), pl.ds(at, LANES)].T.astype(jnp.bfloat16)
            send[c, pl.ds(plane(dz) * 4, 4), i] = turned.reshape(4, PIECE, LANES)

    def start(c, dz, some=slice(None)):
        for place in places[some]:
            peer = plane(dz) * 4 + place
            if dz == 0 and place is low:
                pltpu.make_async_copy(send.at[c, me], landing(c).at[me], recv_sem.at[c]).start()
            else:
                pltpu.make_async_remote_copy(
                    src_ref=send.at[c, peer], dst_ref=landing(c).at[me], send_sem=send_sem.at[0],
                    recv_sem=recv_sem.at[c], device_id={"zero": peer}, device_id_type=MESH,
                ).start()

    def heard_of(dz):
        upward = down_first if dz < 0 else 1 - down_first
        return news.at[(1 - upward) * 4 + abs(dz) - 1]

    def pass_on(dz):
        side = 1 if dz > 0 else -1
        upward = down_first if side < 0 else 1 - down_first
        target = plane(-side) * 4 + low
        pl.semaphore_signal(
            news.at[(1 - upward) * 4 + abs(dz)], inc=1, device_id={"zero": target}, device_id_type=MESH
        )

    def blocks_in(count, which):
        blocks = held.at[0, :, pl.ds(0, count * LANES)]
        pltpu.make_async_copy(blocks, blocks, block_sem.at[which]).wait()

    blocks_in(2, 2)
    for dz in NEAR[:2]:
        prepare(0, dz)
    to_pair = pltpu.make_async_remote_copy(
        src_ref=mine, dst_ref=other, send_sem=pair_sem.at[0], recv_sem=pair_sem.at[1],
        device_id={"zero": z * 4 + places[2]}, device_id_type=MESH,
    )

    @pl.when(z == 0)
    def _():
        pl.semaphore_wait(barrier, len(near) + BANK - 1)

    @pl.when(z != 0)
    def _():
        pl.semaphore_wait(barrier, len(near))

    for side in (1, -1):
        pl.semaphore_signal(
            news.at[down_first * 4 if side < 0 else (1 - down_first) * 4],
            inc=1, device_id={"zero": plane(side) * 4 + low}, device_id_type=MESH,
        )
    for c in range(EARLY):
        if c > 0:
            load(c).wait()
            for dz in NEAR:
                prepare(c, dz)
        for dz in NEAR:
            if c == 0 and dz == 0:
                load_block(dz).wait()
                prepare(c, dz)
            start(c, dz, slice(None) if dz == 0 else slice(2, None))
    for copy in small:
        copy.wait()
    part = (router[...] * gain[...]).astype(jnp.bfloat16)
    mine[...] = jnp.concatenate([part, part], axis=1)
    to_pair.start()
    for dz in (1, -1, 2, -2, 3, -3, 4, -4):
        pl.semaphore_wait(heard_of(dz), 1)
        if abs(dz) < 4:
            pass_on(dz)
        if abs(dz) > 1 and dz != -4:
            if dz == 2:
                blocks_in(5, 0)
            for c in range(EARLY):
                prepare(c, dz)
        for c in range(EARLY if dz != -4 else 0):
            start(c, dz, slice(None) if abs(dz) > 1 else slice(0, 2))

    @pl.when(z == 0)
    def _():
        to_banks(whole)

    to_pair.wait()
    lower = lax.broadcasted_iota(jnp.int32, (HEADS, LANES), 1) < ROWS
    keep_mine = jnp.where(lower, 0, 1) == core
    mine[...] = jnp.where(
        keep_mine, mine[...].astype(jnp.float32), other[...].astype(jnp.float32)
    ).astype(jnp.bfloat16)

    def column_copy(dz):
        return pltpu.make_async_remote_copy(
            src_ref=mine, dst_ref=column.at[dz // 2], send_sem=column_sem.at[0], recv_sem=column_sem.at[1],
            device_id={"zero": lax.rem(z + dz, 8) * 4 + low}, device_id_type=MESH,
        )

    @pl.when(core == 0)
    def _():
        column[0] = mine[...]
        for dz in (4, 2, 6):
            column_copy(dz).start()

    @pl.when(core == 1)
    def _():
        for dz in (3, 5, 1, 7):
            column_copy(dz).start()

    def column_wait(which):
        @pl.when(core == 0)
        def _():
            pltpu.make_async_copy(column.at[pl.ds(0, 3)], column.at[pl.ds(0, 3)], column_sem.at[which]).wait()

        @pl.when(core == 1)
        def _():
            pltpu.make_async_copy(column, column, column_sem.at[which]).wait()

    def beside_copy(i):
        return pltpu.make_async_remote_copy(
            src_ref=column, dst_ref=beside.at[i], send_sem=beside_sem.at[0], recv_sem=beside_sem.at[1],
            device_id={"zero": z * 4 + places[i]}, device_id_type=MESH,
        )

    def bank_copy(step):
        return pltpu.make_async_remote_copy(
            src_ref=rows, dst_ref=served.at[bank], send_sem=bank_sem.at[0],
            recv_sem=bank_sem.at[1], device_id={"bank": lax.rem(bank + step, BANK)}, device_id_type=MESH,
        )

    def prepare_and_start(c):
        size = EACH * LANES
        pltpu.make_async_copy(gate.at[pl.ds(0, size)], held.at[c], load_sem.at[c]).wait()
        prepare(c, TURNS[0])
        for turn, dz in enumerate(TURNS):
            if turn + 1 < len(TURNS):
                prepare(c, TURNS[turn + 1])
            start(c, dz)

    def arrive(c):
        pltpu.make_async_copy(landing(c), landing(c), recv_sem.at[c]).wait()

    def take(c, kept):
        arrive(c)
        for i in range(EACH):
            p = c * EACH + i
            kept = finish(recv.at[c], i, p, final, 2 * p, 2 * p + 1, kept)
        return kept

    def step(c, kept):
        prepare_and_start(c)
        return take(c - EARLY, kept)

    kept = lax.fori_loop(EARLY, 4, step, jnp.zeros((PIECE, LANES), jnp.float32))
    @pl.when(z == 0)
    def _():
        pl.semaphore_wait(whole, BANK - 1)
        for other_z in range(1, 8):
            pl.semaphore_signal(everyone, inc=1, device_id={"zero": other_z * 4 + low}, device_id_type=MESH)

    prepare_and_start(4)
    column_wait(1)
    for i in range(3):
        beside_copy(i).start()
    kept = take(4 - EARLY, kept)
    prepare_and_start(CHUNKS - 1)
    pltpu.make_async_copy(beside, beside, beside_sem.at[1]).wait()
    for i in range(4):
        side, parity = lax.div(places[i], 2), lax.rem(places[i], 2)
        for j in range(4):
            chip = lax.rem(z + 8 - 2 * j - parity, 8) * 2 + side
            at = pl.ds(pl.multiple_of(chip * LANES, LANES), LANES)
            rows[:, at] = column[j] if i == 3 else beside[i, j]

    @pl.when(z != 0)
    def _():
        pl.semaphore_wait(everyone, 1)

    for peer in range(1, BANK):
        bank_copy(peer).start()
    served[bank] = rows[...]

    scales[...] = lax.fori_loop(CHUNKS - 1 - EARLY, CHUNKS - 1, take, kept)
    column_wait(0)
    pltpu.make_async_copy(beside, beside, beside_sem.at[0]).wait()
    blocks = served.at[pl.ds(0, BANK - 1)]
    pltpu.make_async_copy(blocks, blocks, bank_sem.at[0]).wait()
    pltpu.make_async_copy(blocks, blocks, bank_sem.at[1]).wait()
    arrive(CHUNKS - 1)
    sent = send.at[:, pl.ds(0, ZERO - 1)]
    pltpu.make_async_copy(sent, sent, send_sem.at[0]).wait()


def write_out(
    final, last, scales, served,
    gate, up, down, scale_gate, scale_up, scale_down, router,
    tail, turned, sems,
):
    copies = []

    def put(source, target):
        copy = pltpu.make_async_copy(source, target, sems.at[len(copies)])
        copy.start()
        copies.append(copy)

    put(final.at[pl.ds(0, 8)], gate)
    put(final.at[pl.ds(8, 8)], up)
    put(final.at[pl.ds(16, 4)], down.at[pl.ds(0, 4)])
    put(served, router)
    kept = scales[...]
    for i in range(EACH):
        kept = finish(last, i, PAIRS - EACH + i, tail, 2 * i, 2 * i + 1, kept)
        put(tail.at[pl.ds(2 * i, 2)], down.at[pl.ds(4 + 2 * i, 2)])
    turned[...] = kept.T[: 2 * PAIRS, :]
    for i, target in enumerate((scale_gate, scale_up, scale_down)):
        put(turned.at[pl.ds(i * HEADS, HEADS)], target)
    for copy in copies:
        copy.wait()


def local(master_gate, master_up, master_down, router_weight, router_gain):
    gate = master_gate.reshape(HEADS * ROWS, COLS)
    up = master_up.reshape(HEADS * ROWS, COLS)
    down = jnp.transpose(master_down, (0, 2, 1)).reshape(HEADS * ROWS, COLS)
    router = router_weight.T
    gain = router_gain.reshape(1, ROWS)
    anywhere = pl.BlockSpec(memory_space=pl.ANY)
    vmem = pl.BlockSpec(memory_space=pltpu.VMEM)
    wide = CHIPS * LANES
    held = (
        jax.ShapeDtypeStruct((2 * (PAIRS - EACH), PIECE, wide), jnp.bfloat16),
        jax.ShapeDtypeStruct((ZERO, EACH, PIECE, LANES), jnp.bfloat16),
        jax.ShapeDtypeStruct((PIECE, LANES), jnp.float32),
        jax.ShapeDtypeStruct((BANK, HEADS, wide), jnp.bfloat16),
    )
    final, last, scales, served = pl.pallas_call(
        exchange,
        out_shape=held,
        in_specs=[pl.BlockSpec(memory_space=pltpu.HBM)] * 5,
        out_specs=(vmem,) * 4,
        scratch_shapes=[
            pltpu.VMEM((CHUNKS, EACH * LANES, COLS), jnp.float32),
            pltpu.VMEM((HEADS, ROWS), jnp.float32),
            pltpu.VMEM((1, ROWS), jnp.float32),
            pltpu.VMEM((CHUNKS, ZERO, EACH, PIECE, LANES), jnp.bfloat16),
            pltpu.VMEM((CHUNKS - 1, ZERO, EACH, PIECE, LANES), jnp.bfloat16),
            pltpu.VMEM((HEADS, LANES), jnp.bfloat16),
            pltpu.VMEM((HEADS, LANES), jnp.bfloat16),
            pltpu.VMEM((4, HEADS, LANES), jnp.bfloat16),
            pltpu.VMEM((3, 4, HEADS, LANES), jnp.bfloat16),
            pltpu.VMEM((HEADS, wide), jnp.bfloat16),
            pltpu.SemaphoreType.DMA((CHUNKS,)),
            pltpu.SemaphoreType.DMA((1,)),
            pltpu.SemaphoreType.DMA((CHUNKS,)),
            pltpu.SemaphoreType.DMA((2,)),
            pltpu.SemaphoreType.DMA((2,)),
            pltpu.SemaphoreType.DMA((2,)),
            pltpu.SemaphoreType.DMA((2,)),
            pltpu.SemaphoreType.DMA((2,)),
            pltpu.SemaphoreType.REGULAR((8,)),
            pltpu.SemaphoreType.DMA((3,)),
            pltpu.SemaphoreType.REGULAR,
            pltpu.SemaphoreType.REGULAR,
        ],
        compiler_params=pltpu.CompilerParams(
            collective_id=0, has_side_effects=True, vmem_limit_bytes=24 * 2**20
        ),
        name="exchange",
    )(*(pltpu.with_memory_space_constraint(a, pltpu.HBM) for a in (gate, up, down, router, gain)))
    piece = jax.ShapeDtypeStruct((HEADS, PIECE, wide), jnp.bfloat16)
    scale = jax.ShapeDtypeStruct((HEADS, PIECE), jnp.float32)
    outs = pl.pallas_call(
        write_out,
        out_shape=(piece, piece, piece, scale, scale, scale, held[3]),
        in_specs=[vmem] * 4,
        out_specs=(anywhere,) * 7,
        scratch_shapes=[
            pltpu.VMEM((2 * EACH, PIECE, wide), jnp.bfloat16),
            pltpu.VMEM((2 * PAIRS, PIECE), jnp.float32),
            pltpu.SemaphoreType.DMA((9,)),
        ],
        compiler_params=pltpu.CompilerParams(vmem_limit_bytes=8 * 2**20),
        name="write_out",
    )(final, last, scales, served)
    final_gate, final_up, final_down, scale_gate, scale_up, scale_down, router_out = outs
    serve_router = router_out.reshape(BANK * HEADS, wide).T
    return (
        jnp.transpose(final_gate, (0, 2, 1)), jnp.transpose(final_up, (0, 2, 1)), final_down,
        scale_gate, scale_up, scale_down, serve_router,
    )


def solution(mesh):
    in_specs = (
        P("bank", "zero", None),
        P("bank", "zero", None),
        P("bank", None, "zero"),
        P("zero", "bank"),
        P("zero"),
    )
    out_specs = (
        P("bank", None, "zero"),
        P("bank", None, "zero"),
        P("bank", "zero", None),
        P("bank", "zero"),
        P("bank", "zero"),
        P("bank", "zero"),
        P(),
    )
    return jax.shard_map(local, mesh=mesh, in_specs=in_specs, out_specs=out_specs, check_vma=False)
```
